32 devices in a mesh: row: 8 (over z, y), col: 4 (over x, core).
Axes of the slice: x: 2, y: 2, z: 4, core: 2. Of those that a mesh axis runs over, the one named last changes fastest.
Arguments:
- features: bfloat16 [6144, 4096], P(('row', 'col')), may hold values from -6 to 6
- cotangent: bfloat16 [6144, 8192], P(('row', 'col')), may hold values from -0.078125 to 0.078125
Outputs:
- weight_grad: float32 [4096, 8192], P('row', 'col')
The draws below stay inside these ranges and needn't reach their ends.
All inputs are finite; a program needn't handle non-finite values.
Results may differ from the reference program's by a relative error of at most 0.0003.
Values may be sent and summed in bfloat16 or wider, within the bound.
A program may use at most 256 MiB of HBM per device.

```python
import jax
import jax.numpy as jnp
from jax import lax

DIN = 4096
DOUT = 8192
TOK_DEV = 192
TOKENS = 6144
N_ROW = 8
N_COL = 4


def strengthened(array, rng, source, target, blocks, factor):
    owner, partner = [(jnp.arange(array.shape[position]) // (array.shape[position] // blocks)).reshape([-1 if axis == position else 1 for axis in range(array.ndim)]) for position in (source, target)]
    chosen = jax.random.permutation(rng, blocks)[partner]
    strong = (owner == chosen) | (owner == (partner + blocks // 2) % blocks)
    return jnp.where(strong, factor * array, array)


def block_levels(own_key, extent, split, low, high):
    def one(position, shards_of):
        heights = jax.random.uniform(jax.random.fold_in(jax.random.fold_in(own_key, 6), position), (shards_of,), jnp.float32, low / len(split), high / len(split))
        return jnp.repeat(jnp.exp(heights), extent[position] // shards_of).reshape((-1,) + (1,) * (len(extent) - position - 1))

    level = one(*split[0])
    for cut in split[1:]:
        level = level * one(*cut)
    return level


def centred(stream_key, shape, width, most, cuts=(), dtype=jnp.bfloat16):
    values = jax.random.normal(stream_key, shape, jnp.float32) * width
    if len(cuts) > 0:
        values = block_levels(stream_key, shape, cuts, -0.22, 0.18) * values
    return jnp.clip(values, min=-most, max=most).astype(dtype)


def heavy_noise(key, shape, deviation, bound, shards, heavy, kind=jnp.bfloat16):
    drawn = deviation * jax.random.normal(key, shape, jnp.float32)
    if shards:
        drawn = drawn * block_levels(key, shape, shards, -0.22, 0.18)
    return jnp.clip(strengthened(drawn, jax.random.fold_in(key, 3), *heavy), -bound, bound).astype(kind)


def setup_inputs(seed: int = 0) -> dict:
    key_of = jax.random.split(jax.random.key(seed), 3)
    features = heavy_noise(key_of[0], (TOKENS, DIN), 1.0, 6.0, ((0, 32),), (0, 1, 32, 2.75))
    cotangent = centred(key_of[1], (TOKENS, DOUT), TOKENS ** -0.5, 0.078125, ((0, 32),))
    return {"features": features, "cotangent": cotangent}


def reference(features, cotangent):
    block_rows = TOK_DEV * N_COL
    feature_blocks = features.reshape(N_ROW, block_rows, DIN)
    cotangent_blocks = cotangent.reshape(N_ROW, block_rows, DOUT)

    def accumulate(running, paired):
        left = paired[0].astype(jnp.float32)
        right = paired[1].astype(jnp.float32)
        return running + jnp.dot(left.T, right, precision=lax.Precision.HIGHEST), None

    initial = jnp.zeros((DIN, DOUT), jnp.float32)
    weight_grad, unused = lax.scan(accumulate, initial, (feature_blocks, cotangent_blocks))
    return weight_grad
```

```python
import functools

import jax
import jax.numpy as jnp
from jax import lax
from jax.experimental import pallas as pl
from jax.experimental.pallas import tpu as pltpu
from jax.sharding import PartitionSpec as P

MESH = pl.DeviceIdType.MESH
CHUNK = 256
VMEM_MOST = 60 * 1024 * 1024


def tokens_product(left, right):
    return lax.dot_general(
        left, right, (((0,), (0,)), ((), ())), preferred_element_type=jnp.float32
    )


def plain(features, cotangent):
    row_count = lax.axis_size("row")
    width_in = features.shape[1]
    local_rows = width_in // row_count
    columns = lax.all_to_all(cotangent, "col", split_axis=1, concat_axis=0, tiled=True)
    tok_local = features.shape[0]
    exchanged = lax.all_to_all(features, "row", split_axis=1, concat_axis=0, tiled=True)
    stacked = exchanged.reshape(row_count, tok_local, local_rows)
    gathered = lax.all_gather(stacked, "col", axis=1, tiled=True)
    all_tokens = gathered.reshape(-1, local_rows)
    return tokens_product(all_tokens, lax.all_gather(columns, "row", axis=0, tiled=True))


def kernel(
    lines, cols, feat, cot, out,
    fall, dall, ysend, yrecv, acc,
    f_loc, d_loc, fz_s, fz_r, fx_s, fx_r, dx_s, dx_r, rz_s, lz_s, z_r, y_s, y_r, o_s,
):
    row = lax.axis_index("row")
    col = lax.axis_index("col")
    z, y = row // 2, row % 2
    tok = feat.shape[0]
    rows = fall.shape[1]
    half = rows // 2
    chunks = dall.shape[0]
    width = chunks * CHUNK
    plane = tok * cols

    def at_z(other):
        return {"row": other * 2 + y, "col": col}

    def at_col(other):
        return {"row": row, "col": other}

    partner = {"row": z * 2 + (1 - y), "col": col}

    def remote(src, dst, s, r, dev):
        return pltpu.make_async_remote_copy(
            src_ref=src, dst_ref=dst, send_sem=s, recv_sem=r,
            device_id=dev, device_id_type=MESH,
        )

    barrier = pltpu.get_barrier_semaphore()
    for d in range(1, lines):
        pl.semaphore_signal(barrier, inc=1, device_id=at_z((z + d) % lines), device_id_type=MESH)
    for d in range(1, cols):
        pl.semaphore_signal(barrier, inc=1, device_id=at_col((col + d) % cols), device_id_type=MESH)
    pl.semaphore_signal(barrier, inc=1, device_id=partner, device_id_type=MESH)
    pl.semaphore_wait(barrier, lines + cols - 1)

    def mine(zz, cc):
        return pl.ds(pl.multiple_of((zz * cols + cc) * tok, tok), tok)

    def f_cols(zz):
        return feat.at[:, pl.ds(pl.multiple_of(zz * rows, rows), rows)]

    def f_send(zz):
        return remote(f_cols(zz), fall.at[mine(z, col)], fz_s.at[zz], fz_r.at[z], at_z(zz))

    def f_recv(zz):
        return remote(f_cols(z), fall.at[mine(zz, col)], fz_s.at[zz], fz_r.at[zz], at_z(zz))

    def f_gather(zz, d):
        to = (col + d) % cols
        return remote(
            fall.at[mine(zz, col)], fall.at[mine(zz, col)],
            fx_s.at[zz, d], fx_r.at[zz, d], at_col(to),
        )

    def f_gathered(zz, d):
        block = fall.at[mine(zz, (col + cols - d) % cols)]
        return remote(block, block, fx_s.at[zz, d], fx_r.at[zz, d], at_col((col + d) % cols))

    def d_cols(cc, j):
        return cot.at[:, pl.ds(pl.multiple_of(cc * width + j * CHUNK, CHUNK), CHUNK)]

    def d_send(j, d):
        to = (col + d) % cols
        return remote(
            d_cols(to, j), dall.at[j, mine(z, col)], dx_s.at[j, d], dx_r.at[j, d], at_col(to)
        )

    def d_recv(j, d):
        block = dall.at[j, mine(z, (col + cols - d) % cols)]
        return remote(block, block, dx_s.at[j, d], dx_r.at[j, d], at_col((col + d) % cols))

    def plane_of(j, zz):
        return dall.at[j, pl.ds(pl.multiple_of(zz * plane, plane), plane)]

    def z_right(j, zz):
        return remote(plane_of(j, zz), plane_of(j, zz), rz_s.at[j, zz], z_r.at[j, zz], at_z((z + 1) % lines))

    def z_left(j, zz):
        return remote(plane_of(j, zz), plane_of(j, zz), lz_s.at[j, zz], z_r.at[j, zz], at_z((z + lines - 1) % lines))

    f_own = pltpu.make_async_copy(f_cols(z), fall.at[mine(z, col)], f_loc)
    f_own.start()
    for j in range(chunks):
        pltpu.make_async_copy(d_cols(col, j), dall.at[j, mine(z, col)], d_loc.at[j]).start()
    for d in range(lines - 1, 0, -1):
        for zz in (z + d, z - d):
            @pl.when((zz >= 0) & (zz < lines))
            def _():
                f_send(zz).start()
    for j in range(chunks):
        for d in range(1, cols):
            d_send(j, d).start()

    def send_own(j):
        pltpu.make_async_copy(d_cols(col, j), dall.at[j, mine(z, col)], d_loc.at[j]).wait()
        for d in range(1, cols):
            d_recv(j, d).wait_recv()

        @pl.when(z < lines - 1)
        def _():
            z_right(j, z).start()

        @pl.when(z > 0)
        def _():
            z_left(j, z).start()

    def relay(j):
        for d in range(1, lines):
            @pl.when(z - d >= 0)
            def _():
                z_right(j, z - d).wait_recv()

                @pl.when(z < lines - 1)
                def _():
                    z_right(j, z - d).start()

            @pl.when(z + d < lines)
            def _():
                z_left(j, z + d).wait_recv()

                @pl.when(z > 0)
                def _():
                    z_left(j, z + d).start()

    tile = min(CHUNK, half)

    def product(j, into, which):
        @pl.loop(0, half // tile)
        def _(m):
            start = pl.multiple_of(which * half + m * tile, tile)
            into[j, pl.ds(pl.multiple_of(m * tile, tile), tile), :] = tokens_product(
                fall[:, pl.ds(start, tile)], dall[j]
            )

    def y_copy(j):
        return remote(ysend.at[j], yrecv.at[j], y_s.at[j], y_r.at[j], partner)

    def out_copy(j):
        return pltpu.make_async_copy(acc.at[j], out.at[:, pl.ds(j * CHUNK, CHUNK)], o_s.at[j])

    def multiply(j):
        product(j, ysend, 1 - y)
        product(j, acc, y)
        y_copy(j).start()

    def finish(j):
        y_copy(j).wait()
        acc[j] += yrecv[j]
        out_copy(j).start()

    ahead = min(2, chunks)
    for j in range(ahead):
        send_own(j)
    f_own.wait()
    for d in range(1, cols):
        f_gather(z, d).start()
    for dz in range(1, lines):
        zz = (z + dz) % lines
        f_recv(zz).wait_recv()
        for d in range(1, cols):
            f_gather(zz, d).start()

    begin = min(3, chunks - 1)
    done = 0
    finished = 0
    for i in range(chunks):
        if i + ahead < chunks:
            send_own(i + ahead)
        relay(i)
        if i < begin:
            continue
        if done == 0:
            for zz in range(lines):
                for d in range(1, cols):
                    f_gathered(zz, d).wait_recv()
        upto = min(i + 1, done + 2) if i < chunks - 1 else chunks
        before = done
        while done < upto:
            multiply(done)
            done += 1
        while finished < before:
            finish(finished)
            finished += 1
    while finished < chunks:
        finish(finished)
        finished += 1

    for j in range(chunks):
        out_copy(j).wait()
        for d in range(1, cols):
            d_send(j, d).wait_send()
        for d in range(lines):
            @pl.when((z - d >= 0) & (z < lines - 1))
            def _():
                z_right(j, z - d).wait_send()

            @pl.when((z + d < lines) & (z > 0))
            def _():
                z_left(j, z + d).wait_send()
    for dz in range(1, lines):
        f_send((z + dz) % lines).wait_send()
    for zz in range(lines):
        for d in range(1, cols):
            f_gather(zz, d).wait_send()


def fused(row_count, cols, features, cotangent):
    lines = row_count // 2
    tok = features.shape[0]
    rows = features.shape[1] // lines
    width = cotangent.shape[1] // cols
    chunks = width // CHUNK
    tokens = tok * cols * lines
    half = rows // 2
    dma = pltpu.SemaphoreType.DMA
    return pl.pallas_call(
        functools.partial(kernel, lines, cols),
        out_shape=jax.ShapeDtypeStruct((half, width), jnp.float32),
        in_specs=[pl.BlockSpec(memory_space=pl.ANY)] * 2,
        out_specs=pl.BlockSpec(memory_space=pl.ANY),
        scratch_shapes=[
            pltpu.VMEM((tokens, rows), jnp.bfloat16),
            pltpu.VMEM((chunks, tokens, CHUNK), jnp.bfloat16),
            pltpu.VMEM((chunks, half, CHUNK), jnp.float32),
            pltpu.VMEM((chunks, half, CHUNK), jnp.float32),
            pltpu.VMEM((chunks, half, CHUNK), jnp.float32),
            dma(()), dma((chunks,)),
            dma((lines,)), dma((lines,)),
            dma((lines, cols)), dma((lines, cols)),
            dma((chunks, cols)), dma((chunks, cols)),
            dma((chunks, lines)), dma((chunks, lines)), dma((chunks, lines)),
            dma((chunks,)), dma((chunks,)), dma((chunks,)),
        ],
        compiler_params=pltpu.CompilerParams(
            collective_id=0, has_side_effects=True, vmem_limit_bytes=VMEM_MOST
        ),
    )(features, cotangent)


def fits(row_count, cols, features, cotangent):
    if row_count % 2 or cotangent.shape[1] % (cols * CHUNK):
        return False
    if features.shape[1] % (row_count * 128):
        return False
    lines = row_count // 2
    tokens = features.shape[0] * cols * lines
    rows = features.shape[1] // lines
    width = cotangent.shape[1] // cols
    held = 2 * tokens * (rows + width) + 6 * rows * width
    return lines > 1 and cols > 1 and held <= VMEM_MOST * 3 // 4


def local(row_count, cols, features, cotangent):
    if fits(row_count, cols, features, cotangent):
        return fused(row_count, cols, features, cotangent)
    return plain(features, cotangent)


def solution(mesh):
    placed = (P(("row", "col"), None), P(("row", "col"), None))
    body = functools.partial(local, mesh.shape["row"], mesh.shape["col"])
    return jax.shard_map(
        body, mesh=mesh, in_specs=placed, out_specs=P("row", "col"), check_vma=False
    )
```

```python
import functools

import jax
import jax.numpy as jnp
from jax import lax
from jax.experimental import pallas as pl
from jax.experimental.pallas import tpu as pltpu
from jax.sharding import PartitionSpec as P

MESH = pl.DeviceIdType.MESH
CHUNK = 256
AHEAD = 3
LAG = 3
E_LAG = 2
VMEM_MOST = 60 * 1024 * 1024


def tokens_product(left, right):
    return lax.dot_general(
        left, right, (((0,), (0,)), ((), ())), preferred_element_type=jnp.float32
    )


def plain(features, cotangent):
    row_count = lax.axis_size("row")
    width_in = features.shape[1]
    local_rows = width_in // row_count
    columns = lax.all_to_all(cotangent, "col", split_axis=1, concat_axis=0, tiled=True)
    tok_local = features.shape[0]
    exchanged = lax.all_to_all(features, "row", split_axis=1, concat_axis=0, tiled=True)
    stacked = exchanged.reshape(row_count, tok_local, local_rows)
    gathered = lax.all_gather(stacked, "col", axis=1, tiled=True)
    all_tokens = gathered.reshape(-1, local_rows)
    return tokens_product(all_tokens, lax.all_gather(columns, "row", axis=0, tiled=True))


def partial_chunks(chunks):
    return tuple(j for j in range(2, chunks - 1) if j % 3 != 1)


def kernel(
    lines, cols, part, feat, cot, out,
    fall, fend, dall, ysend, yrecv, acc, esend, erecv, eacc, eland,
    f_loc, d_loc, fz_s, fz_r, f2_r, fr_s, gx_s, gx_r, gm_s, gm_r, dx_s, dx_r,
    rz_s, lz_s, z_r, y_s, y_r, ey_s, ey_r, ez_s, ez_r, o_s,
):
    row = lax.axis_index("row")
    col = lax.axis_index("col")
    z, y = row // 2, row % 2
    tok = feat.shape[0]
    rows = fall.shape[1]
    half = rows // 2
    chunks = dall.shape[0]
    width = chunks * CHUNK
    plane = tok * cols
    chips = cols // 2
    mate = col + 1 - 2 * (col % 2)
    last = lines - 1
    is_end = (z == 0) | (z == last)
    helps = (z == 1) | (z == last - 1)
    end = jnp.where(z * 2 < lines, 0, last)

    def at_z(other):
        return {"row": other * 2 + y, "col": col}

    def at_col(other):
        return {"row": row, "col": other}

    partner = {"row": z * 2 + (1 - y), "col": col}

    def remote(src, dst, s, r, dev):
        return pltpu.make_async_remote_copy(
            src_ref=src, dst_ref=dst, send_sem=s, recv_sem=r,
            device_id=dev, device_id_type=MESH,
        )

    barrier = pltpu.get_barrier_semaphore()
    for d in range(1, lines):
        pl.semaphore_signal(barrier, inc=1, device_id=at_z((z + d) % lines), device_id_type=MESH)
    for d in range(1, cols):
        pl.semaphore_signal(barrier, inc=1, device_id=at_col((col + d) % cols), device_id_type=MESH)
    pl.semaphore_signal(barrier, inc=1, device_id=partner, device_id_type=MESH)
    pl.semaphore_wait(barrier, lines + cols - 1)

    def mine(zz, cc):
        return pl.ds(pl.multiple_of((zz * cols + cc) * tok, tok), tok)

    def f_cols(zz):
        return feat.at[:, pl.ds(pl.multiple_of(zz * rows, rows), rows)]

    def f_send(zz):
        return remote(f_cols(zz), fall.at[mine(z, col)], fz_s.at[zz], fz_r.at[z], at_z(zz))

    def f_send_end(zz):
        to = jnp.where(zz == 0, 1, last - 1)
        return remote(f_cols(zz), fend.at[mine(z, col)], fz_s.at[zz], f2_r.at[z], at_z(to))

    def f_recv(zz):
        return remote(f_cols(z), fall.at[mine(zz, col)], fz_s.at[zz], fz_r.at[zz], at_z(zz))

    def f_recv_end(zz):
        return remote(f_cols(z), fend.at[mine(zz, col)], fz_s.at[zz], f2_r.at[zz], at_z(zz))

    def f_relay(zz):
        return remote(
            fend.at[mine(zz, col)], fall.at[mine(zz, col)], fr_s.at[zz], fz_r.at[zz], at_z(end)
        )

    held = (fall, fend)

    def g_send(b, zz, k):
        block = held[b].at[mine(zz, col)]
        return remote(
            block, block, gx_s.at[b, zz, k], gx_r.at[b, zz, k], at_col((col + 2 * k) % cols)
        )

    def g_recv(b, zz, k):
        block = held[b].at[mine(zz, (col + cols - 2 * k) % cols)]
        return remote(
            block, block, gx_s.at[b, zz, k], gx_r.at[b, zz, k], at_col((col + 2 * k) % cols)
        )

    def m_send(b, zz, k):
        block = held[b].at[mine(zz, (col + cols - 2 * k) % cols)]
        return remote(block, block, gm_s.at[b, zz, k], gm_r.at[b, zz, k], at_col(mate))

    def m_recv(b, zz, k):
        block = held[b].at[mine(zz, (mate + cols - 2 * k) % cols)]
        return remote(block, block, gm_s.at[b, zz, k], gm_r.at[b, zz, k], at_col(mate))

    def gather_start(b, zz):
        for k in range(1, chips):
            g_send(b, zz, k).start()
        m_send(b, zz, 0).start()

    def gather_forward(b, zz):
        for k in range(1, chips):
            g_recv(b, zz, k).wait_recv()
            m_send(b, zz, k).start()

    def gather_end(b, zz):
        for k in range(chips):
            m_recv(b, zz, k).wait_recv()

    def gather_drain(b, zz):
        for k in range(1, chips):
            g_send(b, zz, k).wait_send()
        for k in range(chips):
            m_send(b, zz, k).wait_send()

    def d_cols(cc, j):
        return cot.at[:, pl.ds(pl.multiple_of(cc * width + j * CHUNK, CHUNK), CHUNK)]

    def d_send(j, d):
        to = (col + d) % cols
        return remote(
            d_cols(to, j), dall.at[j, mine(z, col)], dx_s.at[j, d], dx_r.at[j, d], at_col(to)
        )

    def d_recv(j, d):
        block = dall.at[j, mine(z, (col + cols - d) % cols)]
        return remote(block, block, dx_s.at[j, d], dx_r.at[j, d], at_col((col + d) % cols))

    def plane_of(j, zz):
        return dall.at[j, pl.ds(pl.multiple_of(zz * plane, plane), plane)]

    def z_right(j, zz):
        return remote(plane_of(j, zz), plane_of(j, zz), rz_s.at[j, zz], z_r.at[j, zz], at_z((z + 1) % lines))

    def z_left(j, zz):
        return remote(plane_of(j, zz), plane_of(j, zz), lz_s.at[j, zz], z_r.at[j, zz], at_z((z + last) % lines))

    def most(j):
        return last - 1 if j in part else last

    def least(j):
        return 1 if j in part else 0

    f_own = pltpu.make_async_copy(f_cols(z), fall.at[mine(z, col)], f_loc.at[0])
    f_own.start()
    f_own_end = pltpu.make_async_copy(f_cols(end), fend.at[mine(z, col)], f_loc.at[1])

    @pl.when(helps)
    def _():
        f_own_end.start()

    for j in range(chunks):
        pltpu.make_async_copy(d_cols(col, j), dall.at[j, mine(z, col)], d_loc.at[j]).start()

    def by_helper(zz):
        return ((zz == 0) & (z != 1)) | ((zz == last) & (z != last - 1))

    for via in (False, True):
        for d in range(last, 0, -1):
            for zz in (z + d, z - d):
                inside = (zz >= 0) & (zz < lines)

                @pl.when(inside & by_helper(zz) if via else inside & ~by_helper(zz))
                def _():
                    (f_send_end if via else f_send)(zz).start()

    ahead = min(AHEAD, chunks)
    for j in range(ahead):
        for d in range(1, cols):
            d_send(j, d).start()
    f_own.wait()
    gather_start(0, z)

    def send_own(j):
        pltpu.make_async_copy(d_cols(col, j), dall.at[j, mine(z, col)], d_loc.at[j]).wait()
        for d in range(1, cols):
            d_recv(j, d).wait_recv()

        @pl.when(z < most(j))
        def _():
            z_right(j, z).start()

        @pl.when(z > least(j))
        def _():
            z_left(j, z).start()

    def relay(j):
        for d in range(1, lines):
            @pl.when((z - d >= 0) & (z <= most(j)))
            def _():
                z_right(j, z - d).wait_recv()

                @pl.when(z < most(j))
                def _():
                    z_right(j, z - d).start()

            @pl.when((z + d < lines) & (z >= least(j)))
            def _():
                z_left(j, z + d).wait_recv()

                @pl.when(z > least(j))
                def _():
                    z_left(j, z + d).start()

    tile = min(CHUNK, half)

    def product(left, j, into, at, which, start, length):
        span = pl.ds(pl.multiple_of(start, plane), length)

        @pl.loop(0, half // tile)
        def _(m):
            begin = pl.multiple_of(which * half + m * tile, tile)
            into[at, pl.ds(pl.multiple_of(m * tile, tile), tile), :] = tokens_product(
                left[span, pl.ds(begin, tile)], dall[j, span]
            )

    def y_copy(j):
        return remote(ysend.at[j], yrecv.at[j], y_s.at[j], y_r.at[j], partner)

    def out_copy(j):
        return pltpu.make_async_copy(acc.at[j], out.at[:, pl.ds(j * CHUNK, CHUNK)], o_s.at[j])

    def multiply(j):
        if j in part:
            @pl.when(is_end)
            def _():
                product(fall, j, ysend, j, 1 - y, z * plane, plane)
                product(fall, j, acc, j, y, z * plane, plane)

            @pl.when(~is_end)
            def _():
                product(fall, j, ysend, j, 1 - y, 0, lines * plane)
                product(fall, j, acc, j, y, 0, lines * plane)
        else:
            product(fall, j, ysend, j, 1 - y, 0, lines * plane)
            product(fall, j, acc, j, y, 0, lines * plane)
        y_copy(j).start()

    def finish(j):
        y_copy(j).wait()
        acc[j] += yrecv[j]
        if j in part:
            @pl.when(~is_end)
            def _():
                out_copy(j).start()
        else:
            out_copy(j).start()

    def e_copy(p):
        return remote(esend.at[p], erecv.at[p], ey_s.at[p], ey_r.at[p], partner)

    def e_move(p):
        return remote(eacc.at[p], eland.at[p], ez_s.at[p], ez_r.at[p], at_z(end))

    def extra(p):
        @pl.when(helps)
        def _():
            start = jnp.where(end == 0, plane, 0)
            product(fend, part[p], esend, p, 1 - y, start, last * plane)
            product(fend, part[p], eacc, p, y, start, last * plane)
            e_copy(p).start()

    def extra_finish(p):
        @pl.when(helps)
        def _():
            e_copy(p).wait()
            eacc[p] += erecv[p]
            e_move(p).start()

    for j in range(ahead):
        send_own(j)
    for dz in range(1, lines):
        zz = (z + dz) % lines

        @pl.when(~is_end)
        def _():
            f_recv(zz).wait_recv()
            gather_start(0, zz)
    for j in range(ahead, chunks):
        for d in range(1, cols):
            d_send(j, d).start()

    @pl.when(helps)
    def _():
        f_own_end.wait()
        gather_start(1, z)
        for dz in range(1, lines):
            zz = (z + dz) % lines

            @pl.when(zz != end)
            def _():
                f_recv_end(zz).wait_recv()
                f_relay(zz).start()
                gather_start(1, zz)

    @pl.when(is_end)
    def _():
        for dz in range(1, lines):
            zz = (z + dz) % lines
            f_recv(zz).wait_recv()
            gather_start(0, zz)

    finished = 0
    e_finished = 0
    for i in range(chunks):
        if i + ahead < chunks:
            send_own(i + ahead)
        relay(i)
        if i == 0:
            for zz in range(lines):
                gather_forward(0, zz)
            for zz in range(lines):
                gather_end(0, zz)
        if i == min(2, chunks - 1):
            for step in (gather_forward, gather_end):
                for zz in range(lines):
                    @pl.when(helps & (zz != end))
                    def _():
                        step(1, zz)
        if i in part:
            extra(part.index(i))
        multiply(i)
        if e_finished < len(part) and part[e_finished] + E_LAG <= i:
            extra_finish(e_finished)
            e_finished += 1
        if i >= LAG:
            finish(finished)
            finished += 1
    while e_finished < len(part):
        extra_finish(e_finished)
        e_finished += 1
    while finished < chunks:
        finish(finished)
        finished += 1
    for p, j in enumerate(part):
        @pl.when(is_end)
        def _():
            e_move(p).wait_recv()
            acc[j] += eland[p]
            out_copy(j).start()

    for j in range(chunks):
        out_copy(j).wait()
        for d in range(1, cols):
            d_send(j, d).wait_send()
        for d in range(lines):
            @pl.when((z - d >= 0) & (z < most(j)))
            def _():
                z_right(j, z - d).wait_send()

            @pl.when((z + d < lines) & (z > least(j)))
            def _():
                z_left(j, z + d).wait_send()
    for dz in range(1, lines):
        f_send((z + dz) % lines).wait_send()
    for zz in range(lines):
        gather_drain(0, zz)

        @pl.when(helps & (zz != end))
        def _():
            gather_drain(1, zz)

            @pl.when(zz != z)
            def _():
                f_relay(zz).wait_send()
    for p in range(len(part)):
        @pl.when(helps)
        def _():
            e_move(p).wait_send()


def fused(row_count, cols, features, cotangent):
    lines = row_count // 2
    tok = features.shape[0]
    rows = features.shape[1] // lines
    width = cotangent.shape[1] // cols
    chunks = width // CHUNK
    part = partial_chunks(chunks)
    tokens = tok * cols * lines
    half = rows // 2
    parts = max(len(part), 1)
    dma = pltpu.SemaphoreType.DMA
    whole = pltpu.VMEM((chunks, half, CHUNK), jnp.float32)
    some = pltpu.VMEM((parts, half, CHUNK), jnp.float32)
    return pl.pallas_call(
        functools.partial(kernel, lines, cols, part),
        out_shape=jax.ShapeDtypeStruct((half, width), jnp.float32),
        in_specs=[pl.BlockSpec(memory_space=pl.ANY)] * 2,
        out_specs=pl.BlockSpec(memory_space=pl.ANY),
        scratch_shapes=[
            pltpu.VMEM((tokens, rows), jnp.bfloat16),
            pltpu.VMEM((tokens, rows), jnp.bfloat16),
            pltpu.VMEM((chunks, tokens, CHUNK), jnp.bfloat16),
            whole, whole, whole, some, some, some, some,
            dma((2,)), dma((chunks,)),
            dma((lines,)), dma((lines,)), dma((lines,)), dma((lines,)),
            dma((2, lines, cols)), dma((2, lines, cols)),
            dma((2, lines, cols)), dma((2, lines, cols)),
            dma((chunks, cols)), dma((chunks, cols)),
            dma((chunks, lines)), dma((chunks, lines)), dma((chunks, lines)),
            dma((chunks,)), dma((chunks,)),
            dma((parts,)), dma((parts,)), dma((parts,)), dma((parts,)),
            dma((chunks,)),
        ],
        compiler_params=pltpu.CompilerParams(
            collective_id=0, has_side_effects=True, vmem_limit_bytes=VMEM_MOST
        ),
    )(features, cotangent)


def fits(row_count, cols, features, cotangent):
    if row_count % 2 or cotangent.shape[1] % (cols * CHUNK):
        return False
    if features.shape[1] % (row_count * 128):
        return False
    lines = row_count // 2
    tokens = features.shape[0] * cols * lines
    rows = features.shape[1] // lines
    width = cotangent.shape[1] // cols
    held = 2 * tokens * (2 * rows + width) + 14 * rows * width
    return lines > 3 and cols % 2 == 0 and held <= VMEM_MOST


def local(row_count, cols, features, cotangent):
    if fits(row_count, cols, features, cotangent):
        return fused(row_count, cols, features, cotangent)
    return plain(features, cotangent)


def solution(mesh):
    placed = (P(("row", "col"), None), P(("row", "col"), None))
    body = functools.partial(local, mesh.shape["row"], mesh.shape["col"])
    return jax.shard_map(
        body, mesh=mesh, in_specs=placed, out_specs=P("row", "col"), check_vma=False
    )
```

```python
import functools

import jax
import jax.numpy as jnp
from jax import lax
from jax.experimental import pallas as pl
from jax.experimental.pallas import tpu as pltpu
from jax.sharding import PartitionSpec as P

MESH = pl.DeviceIdType.MESH
CHUNK = 512
AHEAD = 2
LAG = 1
E_LAG = 1
VMEM_MOST = 60 * 1024 * 1024


def tokens_product(left, right):
    return lax.dot_general(
        left, right, (((0,), (0,)), ((), ())), preferred_element_type=jnp.float32
    )


def plain(features, cotangent):
    row_count = lax.axis_size("row")
    width_in = features.shape[1]
    local_rows = width_in // row_count
    columns = lax.all_to_all(cotangent, "col", split_axis=1, concat_axis=0, tiled=True)
    tok_local = features.shape[0]
    exchanged = lax.all_to_all(features, "row", split_axis=1, concat_axis=0, tiled=True)
    stacked = exchanged.reshape(row_count, tok_local, local_rows)
    gathered = lax.all_gather(stacked, "col", axis=1, tiled=True)
    all_tokens = gathered.reshape(-1, local_rows)
    return tokens_product(all_tokens, lax.all_gather(columns, "row", axis=0, tiled=True))


def partial_chunks(chunks):
    return tuple(j for j in range(2, chunks - 1) if j % 3 != 1)


def kernel(
    lines, cols, part, feat, cot, out,
    fall, fend, dall, ysend, yrecv, acc, esend, erecv, eacc, eland,
    f_loc, d_loc, fz_s, fz_r, f2_r, fr_s, gx_s, gx_r, gm_s, gm_r, dx_s, dx_r,
    rz_s, lz_s, z_r, y_s, y_r, ey_s, ey_r, ez_s, ez_r, o_s,
):
    row = lax.axis_index("row")
    col = lax.axis_index("col")
    z, y = row // 2, row % 2
    tok = feat.shape[0]
    rows = fall.shape[1]
    half = rows // 2
    chunks = dall.shape[0]
    width = chunks * CHUNK
    plane = tok * cols
    chips = cols // 2
    mate = col + 1 - 2 * (col % 2)
    last = lines - 1
    is_end = (z == 0) | (z == last)
    helps = (z == 1) | (z == last - 1)
    end = jnp.where(z * 2 < lines, 0, last)

    def at_z(other):
        return {"row": other * 2 + y, "col": col}

    def at_col(other):
        return {"row": row, "col": other}

    partner = {"row": z * 2 + (1 - y), "col": col}

    def remote(src, dst, s, r, dev):
        return pltpu.make_async_remote_copy(
            src_ref=src, dst_ref=dst, send_sem=s, recv_sem=r,
            device_id=dev, device_id_type=MESH,
        )

    barrier = pltpu.get_barrier_semaphore()
    for d in range(1, lines):
        pl.semaphore_signal(barrier, inc=1, device_id=at_z((z + d) % lines), device_id_type=MESH)
    for d in range(1, cols):
        pl.semaphore_signal(barrier, inc=1, device_id=at_col((col + d) % cols), device_id_type=MESH)
    pl.semaphore_signal(barrier, inc=1, device_id=partner, device_id_type=MESH)
    pl.semaphore_wait(barrier, lines + cols - 1)

    def mine(zz, cc):
        return pl.ds(pl.multiple_of((zz * cols + cc) * tok, tok), tok)

    def f_cols(zz):
        return feat.at[:, pl.ds(pl.multiple_of(zz * rows, rows), rows)]

    def f_send(zz):
        return remote(f_cols(zz), fall.at[mine(z, col)], fz_s.at[zz], fz_r.at[z], at_z(zz))

    def f_send_end(zz):
        to = jnp.where(zz == 0, 1, last - 1)
        return remote(f_cols(zz), fend.at[mine(z, col)], fz_s.at[zz], f2_r.at[z], at_z(to))

    def f_recv(zz):
        return remote(f_cols(z), fall.at[mine(zz, col)], fz_s.at[zz], fz_r.at[zz], at_z(zz))

    def f_recv_end(zz):
        return remote(f_cols(z), fend.at[mine(zz, col)], fz_s.at[zz], f2_r.at[zz], at_z(zz))

    def f_relay(zz):
        return remote(
            fend.at[mine(zz, col)], fall.at[mine(zz, col)], fr_s.at[zz], fz_r.at[zz], at_z(end)
        )

    held = (fall, fend)

    def g_send(b, zz, k):
        block = held[b].at[mine(zz, col)]
        return remote(
            block, block, gx_s.at[b, zz, k], gx_r.at[b, zz, k], at_col((col + 2 * k) % cols)
        )

    def g_recv(b, zz, k):
        block = held[b].at[mine(zz, (col + cols - 2 * k) % cols)]
        return remote(
            block, block, gx_s.at[b, zz, k], gx_r.at[b, zz, k], at_col((col + 2 * k) % cols)
        )

    def m_send(b, zz, k):
        block = held[b].at[mine(zz, (col + cols - 2 * k) % cols)]
        return remote(block, block, gm_s.at[b, zz, k], gm_r.at[b, zz, k], at_col(mate))

    def m_recv(b, zz, k):
        block = held[b].at[mine(zz, (mate + cols - 2 * k) % cols)]
        return remote(block, block, gm_s.at[b, zz, k], gm_r.at[b, zz, k], at_col(mate))

    def gather_start(b, zz):
        for k in range(1, chips):
            g_send(b, zz, k).start()
        m_send(b, zz, 0).start()

    def gather_forward(b, zz):
        for k in range(1, chips):
            g_recv(b, zz, k).wait_recv()
            m_send(b, zz, k).start()

    def gather_end(b, zz):
        for k in range(chips):
            m_recv(b, zz, k).wait_recv()

    def gather_drain(b, zz):
        for k in range(1, chips):
            g_send(b, zz, k).wait_send()
        for k in range(chips):
            m_send(b, zz, k).wait_send()

    def d_cols(cc, j):
        return cot.at[:, pl.ds(pl.multiple_of(cc * width + j * CHUNK, CHUNK), CHUNK)]

    def d_send(j, d):
        to = (col + d) % cols
        return remote(
            d_cols(to, j), dall.at[j, mine(z, col)], dx_s.at[j, d], dx_r.at[j, d], at_col(to)
        )

    def d_recv(j, d):
        block = dall.at[j, mine(z, (col + cols - d) % cols)]
        return remote(block, block, dx_s.at[j, d], dx_r.at[j, d], at_col((col + d) % cols))

    def plane_of(j, zz):
        return dall.at[j, pl.ds(pl.multiple_of(zz * plane, plane), plane)]

    def z_right(j, zz):
        return remote(plane_of(j, zz), plane_of(j, zz), rz_s.at[j, zz], z_r.at[j, zz], at_z((z + 1) % lines))

    def z_left(j, zz):
        return remote(plane_of(j, zz), plane_of(j, zz), lz_s.at[j, zz], z_r.at[j, zz], at_z((z + last) % lines))

    def most(j):
        return last - 1 if j in part else last

    def least(j):
        return 1 if j in part else 0

    f_own = pltpu.make_async_copy(f_cols(z), fall.at[mine(z, col)], f_loc.at[0])
    f_own.start()
    f_own_end = pltpu.make_async_copy(f_cols(end), fend.at[mine(z, col)], f_loc.at[1])

    @pl.when(helps)
    def _():
        f_own_end.start()

    for j in range(chunks):
        pltpu.make_async_copy(d_cols(col, j), dall.at[j, mine(z, col)], d_loc.at[j]).start()

    def by_helper(zz):
        return ((zz == 0) & (z != 1)) | ((zz == last) & (z != last - 1))

    for via in (False, True):
        for d in range(last, 0, -1):
            for zz in (z + d, z - d):
                inside = (zz >= 0) & (zz < lines)

                @pl.when(inside & by_helper(zz) if via else inside & ~by_helper(zz))
                def _():
                    (f_send_end if via else f_send)(zz).start()

    ahead = min(AHEAD, chunks)
    for j in range(ahead):
        for d in range(1, cols):
            d_send(j, d).start()
    f_own.wait()
    gather_start(0, z)

    def send_own(j):
        pltpu.make_async_copy(d_cols(col, j), dall.at[j, mine(z, col)], d_loc.at[j]).wait()
        for d in range(1, cols):
            d_recv(j, d).wait_recv()

        @pl.when(z < most(j))
        def _():
            z_right(j, z).start()

        @pl.when(z > least(j))
        def _():
            z_left(j, z).start()

    def relay(j):
        for d in range(1, lines):
            @pl.when((z - d >= 0) & (z <= most(j)))
            def _():
                z_right(j, z - d).wait_recv()

                @pl.when(z < most(j))
                def _():
                    z_right(j, z - d).start()

            @pl.when((z + d < lines) & (z >= least(j)))
            def _():
                z_left(j, z + d).wait_recv()

                @pl.when(z > least(j))
                def _():
                    z_left(j, z + d).start()

    tile = min(CHUNK, half)

    def product(left, j, into, at, which, start, length):
        span = pl.ds(pl.multiple_of(start, plane), length)

        @pl.loop(0, half // tile)
        def _(m):
            begin = pl.multiple_of(which * half + m * tile, tile)
            into[at, pl.ds(pl.multiple_of(m * tile, tile), tile), :] = tokens_product(
                left[span, pl.ds(begin, tile)], dall[j, span]
            )

    def y_copy(j):
        return remote(ysend.at[j], yrecv.at[j], y_s.at[j], y_r.at[j], partner)

    def out_copy(j):
        return pltpu.make_async_copy(acc.at[j], out.at[:, pl.ds(j * CHUNK, CHUNK)], o_s.at[j])

    def multiply(j):
        if j in part:
            @pl.when(is_end)
            def _():
                product(fall, j, ysend, j, 1 - y, z * plane, plane)
                product(fall, j, acc, j, y, z * plane, plane)

            @pl.when(~is_end)
            def _():
                product(fall, j, ysend, j, 1 - y, 0, lines * plane)
                product(fall, j, acc, j, y, 0, lines * plane)
        else:
            product(fall, j, ysend, j, 1 - y, 0, lines * plane)
            product(fall, j, acc, j, y, 0, lines * plane)
        y_copy(j).start()

    def finish(j):
        y_copy(j).wait()
        acc[j] += yrecv[j]
        if j in part:
            @pl.when(~is_end)
            def _():
                out_copy(j).start()
        else:
            out_copy(j).start()

    def e_copy(p):
        return remote(esend.at[p], erecv.at[p], ey_s.at[p], ey_r.at[p], partner)

    def e_move(p):
        return remote(eacc.at[p], eland.at[p], ez_s.at[p], ez_r.at[p], at_z(end))

    def extra(p):
        @pl.when(helps)
        def _():
            start = jnp.where(end == 0, plane, 0)
            product(fend, part[p], esend, p, 1 - y, start, last * plane)
            product(fend, part[p], eacc, p, y, start, last * plane)
            e_copy(p).start()

    def extra_finish(p):
        @pl.when(helps)
        def _():
            e_copy(p).wait()
            eacc[p] += erecv[p]
            e_move(p).start()

    for j in range(ahead):
        send_own(j)
    for dz in range(1, lines):
        zz = (z + dz) % lines

        @pl.when(~is_end)
        def _():
            f_recv(zz).wait_recv()
            gather_start(0, zz)
    for j in range(ahead, chunks):
        for d in range(1, cols):
            d_send(j, d).start()

    @pl.when(helps)
    def _():
        f_own_end.wait()
        gather_start(1, z)
        for dz in range(1, lines):
            zz = (z + dz) % lines

            @pl.when(zz != end)
            def _():
                f_recv_end(zz).wait_recv()
                f_relay(zz).start()
                gather_start(1, zz)

    @pl.when(is_end)
    def _():
        for dz in range(1, lines):
            zz = (z + dz) % lines
            f_recv(zz).wait_recv()
            gather_start(0, zz)

    finished = 0
    e_finished = 0
    for i in range(chunks):
        if i + ahead < chunks:
            send_own(i + ahead)
        relay(i)
        if i == 0:
            for zz in range(lines):
                gather_forward(0, zz)
            for zz in range(lines):
                gather_end(0, zz)
        if i == min(2, chunks - 1):
            for step in (gather_forward, gather_end):
                for zz in range(lines):
                    @pl.when(helps & (zz != end))
                    def _():
                        step(1, zz)
        if i in part:
            extra(part.index(i))
        multiply(i)
        if e_finished < len(part) and part[e_finished] + E_LAG <= i:
            extra_finish(e_finished)
            e_finished += 1
        if i >= LAG:
            finish(finished)
            finished += 1
    while e_finished < len(part):
        extra_finish(e_finished)
        e_finished += 1
    while finished < chunks:
        finish(finished)
        finished += 1
    for p, j in enumerate(part):
        @pl.when(is_end)
        def _():
            e_move(p).wait_recv()
            acc[j] += eland[p]
            out_copy(j).start()

    for j in range(chunks):
        out_copy(j).wait()
        for d in range(1, cols):
            d_send(j, d).wait_send()
        for d in range(lines):
            @pl.when((z - d >= 0) & (z < most(j)))
            def _():
                z_right(j, z - d).wait_send()

            @pl.when((z + d < lines) & (z > least(j)))
            def _():
                z_left(j, z + d).wait_send()
    for dz in range(1, lines):
        f_send((z + dz) % lines).wait_send()
    for zz in range(lines):
        gather_drain(0, zz)

        @pl.when(helps & (zz != end))
        def _():
            gather_drain(1, zz)

            @pl.when(zz != z)
            def _():
                f_relay(zz).wait_send()
    for p in range(len(part)):
        @pl.when(helps)
        def _():
            e_move(p).wait_send()


def fused(row_count, cols, features, cotangent):
    lines = row_count // 2
    tok = features.shape[0]
    rows = features.shape[1] // lines
    width = cotangent.shape[1] // cols
    chunks = width // CHUNK
    part = partial_chunks(chunks)
    tokens = tok * cols * lines
    half = rows // 2
    parts = max(len(part), 1)
    dma = pltpu.SemaphoreType.DMA
    whole = pltpu.VMEM((chunks, half, CHUNK), jnp.float32)
    some = pltpu.VMEM((parts, half, CHUNK), jnp.float32)
    return pl.pallas_call(
        functools.partial(kernel, lines, cols, part),
        out_shape=jax.ShapeDtypeStruct((half, width), jnp.float32),
        in_specs=[pl.BlockSpec(memory_space=pl.ANY)] * 2,
        out_specs=pl.BlockSpec(memory_space=pl.ANY),
        scratch_shapes=[
            pltpu.VMEM((tokens, rows), jnp.bfloat16),
            pltpu.VMEM((tokens, rows), jnp.bfloat16),
            pltpu.VMEM((chunks, tokens, CHUNK), jnp.bfloat16),
            whole, whole, whole, some, some, some, some,
            dma((2,)), dma((chunks,)),
            dma((lines,)), dma((lines,)), dma((lines,)), dma((lines,)),
            dma((2, lines, cols)), dma((2, lines, cols)),
            dma((2, lines, cols)), dma((2, lines, cols)),
            dma((chunks, cols)), dma((chunks, cols)),
            dma((chunks, lines)), dma((chunks, lines)), dma((chunks, lines)),
            dma((chunks,)), dma((chunks,)),
            dma((parts,)), dma((parts,)), dma((parts,)), dma((parts,)),
            dma((chunks,)),
        ],
        compiler_params=pltpu.CompilerParams(
            collective_id=0, has_side_effects=True, vmem_limit_bytes=VMEM_MOST
        ),
    )(features, cotangent)


def fits(row_count, cols, features, cotangent):
    if row_count % 2 or cotangent.shape[1] % (cols * CHUNK):
        return False
    if features.shape[1] % (row_count * 128):
        return False
    lines = row_count // 2
    tokens = features.shape[0] * cols * lines
    rows = features.shape[1] // lines
    width = cotangent.shape[1] // cols
    held = 2 * tokens * (2 * rows + width) + 14 * rows * width
    return lines > 3 and cols % 2 == 0 and held <= VMEM_MOST


def local(row_count, cols, features, cotangent):
    if fits(row_count, cols, features, cotangent):
        return fused(row_count, cols, features, cotangent)
    return plain(features, cotangent)


def solution(mesh):
    placed = (P(("row", "col"), None), P(("row", "col"), None))
    body = functools.partial(local, mesh.shape["row"], mesh.shape["col"])
    return jax.shard_map(
        body, mesh=mesh, in_specs=placed, out_specs=P("row", "col"), check_vma=False
    )
```
